64 devices in a mesh: rep: 8 (over x, y, core), dp: 8 (over z).
Axes of the slice: x: 2, y: 2, z: 8, core: 2. Of those that a mesh axis runs over, the one named last changes fastest.
The devices are a block of a 4x4x8 slice.
Arguments:
- x: bfloat16 [64, 2048, 640], P(('rep', 'dp')), parts along dimension 0
- dy: bfloat16 [64, 2048, 640], P(('rep', 'dp')), parts along dimension 0
- w_gate: bfloat16 [2, 640, 1792], P(None, 'dp')
- w_up: bfloat16 [2, 640, 1792], P(None, 'dp')
- w_down: bfloat16 [2, 1792, 640], P(None, 'dp')
- m_w_gate: float32 [2, 640, 1792], P(None, 'dp')
- m_w_up: float32 [2, 640, 1792], P(None, 'dp')
- m_w_down: float32 [2, 1792, 640], P(None, 'dp')
- v_w_gate: float32 [2, 640, 1792], P(None, 'dp')
- v_w_up: float32 [2, 640, 1792], P(None, 'dp')
- v_w_down: float32 [2, 1792, 640], P(None, 'dp')
Outputs:
- output 1: bfloat16 [16, 640, 1792], P('rep', 'dp'), parts along dimension 0
- output 2: bfloat16 [16, 640, 1792], P('rep', 'dp'), parts along dimension 0
- output 3: bfloat16 [16, 1792, 640], P('rep', 'dp'), parts along dimension 0
- output 4: float32 [16, 640, 1792], P('rep', 'dp'), parts along dimension 0
- output 5: float32 [16, 640, 1792], P('rep', 'dp'), parts along dimension 0
- output 6: float32 [16, 1792, 640], P('rep', 'dp'), parts along dimension 0
- output 7: float32 [16, 640, 1792], P('rep', 'dp'), parts along dimension 0
- output 8: float32 [16, 640, 1792], P('rep', 'dp'), parts along dimension 0
- output 9: float32 [16, 1792, 640], P('rep', 'dp'), parts along dimension 0
There are 8 independent parts. The reference program is written for one: setup_inputs(seed, part) draws one part's arguments, and reference() takes and returns one part's arrays. A program takes and returns all parts, laid end to end along the dimension named above; an argument that names none is the same for every part.
All inputs are finite; a program needn't handle non-finite values.
Results may differ from the reference program's by a relative error of at most 0.02.
Values are sent between devices in bfloat16 or wider.
A program may use at most 768 MiB of HBM per device.

```python
import jax
import jax.numpy as jnp
from jax import lax

SEQUENCES = 8
TOKENS = 2048
D = 640
FF = 1792
LAYERS = 2
NAMES = ("w_gate", "w_up", "w_down")
SHAPES = {"w_gate": (LAYERS, D, FF), "w_up": (LAYERS, D, FF), "w_down": (LAYERS, FF, D)}


def bump(key, n, height):
    away = (jnp.arange(n, dtype=jnp.int32) - jax.random.randint(key, (), 0, n, jnp.int32)) % n
    return jnp.where(away < n // 8, height, 1.0)


def together(key, own, strength):
    shared = jax.random.normal(key, own.shape[1:], jnp.float32)
    return (own + strength * shared) * lax.rsqrt(1 + strength * strength)


def setup_inputs(seed: int = 0, part: int = 0) -> dict:
    kx, kdy, ka, kb, kz, kf, kh, kl, *keys = jax.random.split(jax.random.key(seed), 8 + 3 * len(NAMES))
    kx, kdy, ka, kb = (jax.random.fold_in(k, part) for k in (kx, kdy, ka, kb))
    kw, km, kv = (keys[i::3] for i in range(3))
    shape = (SEQUENCES, TOKENS, D)
    much_x, much_dy = jax.random.uniform(kz, (2,), jnp.float32, 0.0, 1.0)
    loud = 2.0 ** jax.random.uniform(jax.random.fold_in(kz, 1), (), jnp.float32, -1.0, 2.0)
    layers = 2.0 ** jax.random.uniform(kl, (LAYERS, 1, 1), jnp.float32, -1.0, 1.0)
    x = together(ka, jax.random.normal(kx, shape, jnp.float32), much_x) * bump(kf, D, 4.0)
    dy = together(kb, jax.random.normal(kdy, shape, jnp.float32), much_dy)
    drawn = {"x": x.astype(jnp.bfloat16), "dy": (loud * dy * (SEQUENCES * TOKENS) ** -0.5).astype(jnp.bfloat16)}
    for key, name in zip(kw, NAMES, strict=True):
        w = jax.random.normal(key, SHAPES[name], jnp.float32) * SHAPES[name][1] ** -0.5
        drawn[name] = (w * {"w_gate": 1.0, "w_up": bump(kh, FF, 4.0), "w_down": layers}[name]).astype(jnp.bfloat16)
    for key, name in zip(km, NAMES, strict=True):
        drawn[f"m_{name}"] = 0.1 * jax.random.normal(key, SHAPES[name], jnp.float32)
    for key, name in zip(kv, NAMES, strict=True):
        drawn[f"v_{name}"] = jax.random.uniform(key, SHAPES[name], jnp.float32, 0.005, 0.015)
    return drawn


def matmul(a, w):
    return jnp.dot(a, w, preferred_element_type=jnp.float32).astype(jnp.bfloat16)


def normed(h):
    wide = h.astype(jnp.float32)
    scale = lax.rsqrt(jnp.mean(wide**2, -1, keepdims=True) + 1e-6)
    return (wide * scale).astype(jnp.bfloat16)


def layer(h, w):
    a = normed(h)
    gate = jnp.dot(a, w["w_gate"], preferred_element_type=jnp.float32)
    up = jnp.dot(a, w["w_up"], preferred_element_type=jnp.float32)
    return h + matmul((jax.nn.silu(gate) * up).astype(jnp.bfloat16), w["w_down"])


def adamw(w, m, v, g):
    m = 0.9 * m + 0.1 * g
    v = 0.95 * v + 0.05 * g * g
    step = m * lax.rsqrt(v + 1e-8) + 0.1 * w
    return (w - 0.02 * step).astype(jnp.bfloat16), m, v


def stack(weights, h):
    return lax.scan(lambda h, w: (layer(h, w), None), h, weights)[0]


def reference(x, dy, w_gate, w_up, w_down, m_w_gate, m_w_up, m_w_down, v_w_gate, v_w_up, v_w_down):
    weights = dict(zip(NAMES, (w_gate, w_up, w_down), strict=True))

    def take(so_far, sequence):
        h, by_y = sequence
        _, back = jax.vjp(lambda w: stack(w, h), weights)
        return jax.tree.map(lambda total, term: total + term.astype(jnp.float32), so_far, back(by_y)[0]), None

    none_yet = {name: jnp.zeros(w.shape, jnp.float32) for name, w in weights.items()}
    by_weights, _ = lax.scan(take, none_yet, (x, dy))
    gradients = [by_weights[name].astype(jnp.bfloat16).astype(jnp.float32) for name in NAMES]
    new = [
        adamw(w.astype(jnp.float32), m, v, g)
        for w, m, v, g in zip((w_gate, w_up, w_down), (m_w_gate, m_w_up, m_w_down), (v_w_gate, v_w_up, v_w_down), gradients, strict=True)
    ]
    return tuple(one[which] for which in range(3) for one in new)
```

```python
import functools

import jax
import jax.numpy as jnp
from jax import lax
from jax.experimental import pallas as pl
from jax.experimental.pallas import tpu as pltpu
from jax.sharding import PartitionSpec as P

MESH = pl.DeviceIdType.MESH
F32, BF16 = jnp.float32, jnp.bfloat16
CHUNK = 256
STRIP = 128
TILE = 512
VMEM_BYTES = 67043328


def dot(a, b, dims=((1,), (0,))):
    return lax.dot_general(a, b, (dims, ((), ())), preferred_element_type=F32)


def kernel(n, x_ref, dy_ref, wg_ref, wu_ref, wd_ref, gg_ref, gu_ref, gd_ref,
           h, a, at, dyb, wgu, wdn, ggu, gdn, rgu, rdn, acc, dgu, act,
           local_sem, x_sem, ag_recv, ag_send, pair_recv, pair_send, gu_recv, gu_send, dn_recv, dn_send, out_gu, out_dn):
    layers, rows, ff = wg_ref.shape
    half = wd_ref.shape[1] // 2
    tokens, d = h.shape
    chunks, strips = ff // CHUNK, d // STRIP
    pieces = strips + chunks
    far = n // 2
    z = lax.axis_index("dp")
    me = lax.axis_index("rep")
    core = lax.rem(me, 2)
    partner = me + 1 - 2 * core

    def at_ring(k):
        return lax.rem(z + 2 * n + k, n)

    def cols(c, width):
        return pl.ds(pl.multiple_of(c * width, width), width)

    def span(start, size):
        return pl.ds(pl.multiple_of(start, 16), size)

    loads = []
    for l in range(layers):
        loads.append((wg_ref.at[l], wgu.at[l, 0, span(z * rows, rows)]))
        loads.append((wu_ref.at[l], wgu.at[l, 1, span(z * rows, rows)]))
        loads.append((wd_ref.at[l], wdn.at[l, span(z * 2 * half, 2 * half)]))
    loads.append((dy_ref.at[0], dyb))
    loads = [pltpu.make_async_copy(src, dst, local_sem.at[i]) for i, (src, dst) in enumerate(loads)]
    load_x = pltpu.make_async_copy(x_ref.at[0], h, x_sem)
    for load in loads:
        load.start()
    load_x.start()

    barrier = pltpu.get_barrier_semaphore()
    for step in (1, -1):
        pl.semaphore_signal(barrier, inc=1, device_id={"dp": at_ring(step)}, device_id_type=MESH)
    pl.semaphore_signal(barrier, inc=1, device_id={"rep": partner}, device_id_type=MESH)
    pl.semaphore_wait(barrier, 3)
    for load in loads:
        load.wait()

    def block(l, k, down, origin, count=1):
        if down:
            return wdn.at[l, span(origin * 2 * half + core * half, half * count), cols(k, STRIP)]
        return wgu.at[l, core, span(origin * rows, rows * count), cols(k - strips, CHUNK)]

    def hop(l, k, j, down, s):
        for way, sign in ((0, 1), (1, -1)):
            ref = block(l, k, down, at_ring(-sign * s))

            def ring(slot):
                return pltpu.make_async_remote_copy(
                    src_ref=ref, dst_ref=ref, send_sem=ag_send.at[j], recv_sem=ag_recv.at[way, j, slot],
                    device_id={"dp": at_ring(sign)}, device_id_type=MESH)

            def arrive():
                ring(s - 1).wait_recv()

            def send():
                ring(s).start()

            def share():
                pltpu.make_async_remote_copy(
                    src_ref=ref, dst_ref=ref, send_sem=pair_send.at[j], recv_sem=pair_recv.at[j],
                    device_id={"rep": partner}, device_id_type=MESH).start()

            if s == 0:
                send()
            elif s < far - 1:
                arrive()
                send()
                share()
            elif s == far - 1:
                arrive()
                pl.when(lax.rem(j, 2) == way)(send)
                share()
            else:
                @pl.when(lax.rem(j, 2) == way)
                def _():
                    arrive()
                    share()

    def gather(slot):
        for s in range(far + 1):
            j = slot - s
            l, k = lax.div(j, pieces), lax.rem(j, pieces)
            pl.when((j >= 0) & (j < layers * pieces) & (k < strips))(functools.partial(hop, l, k, j, True, s))
            pl.when((j >= 0) & (j < layers * pieces) & (k >= strips))(functools.partial(hop, l, k, j, False, s))

    def all_of(sem_send, sem_recv, down):
        ref = wdn.at[0, pl.ds(0, (n - 1) * half), pl.ds(0, STRIP)] if down else wgu.at[0, 0, pl.ds(0, (n - 1) * rows), pl.ds(0, CHUNK)]
        return pltpu.make_async_remote_copy(
            src_ref=ref, dst_ref=ref, send_sem=sem_send, recv_sem=sem_recv, device_id={"rep": partner}, device_id_type=MESH)

    def need_strips(l):
        @pl.loop(0, strips)
        def _(k):
            j = l * pieces + k
            all_of(pair_send.at[j], pair_recv.at[j], True).wait_recv()

    def need_chunk(l, c):
        j = l * pieces + strips + c
        all_of(pair_send.at[j], pair_recv.at[j], False).wait_recv()

    def tiles(body, size=TILE):
        @pl.loop(0, tokens // size)
        def _(i):
            body(pl.ds(pl.multiple_of(i * size, size), size))

    def norm():
        def body(t):
            wide = h[t, :].astype(F32)
            scale = lax.rsqrt(jnp.mean(wide * wide, -1, keepdims=True) + 1e-6)
            a[t, :] = (wide * scale).astype(BF16)

        tiles(body, 256)

    def transpose():
        tiles(lambda t: at.__setitem__((slice(None), t), a[t, :].T), 256)

    def zero():
        def body(t):
            acc[t, :] = jnp.zeros((TILE, d), F32)

        tiles(body)

    def gates(l, c, t):
        gate = dot(a[t, :], wgu[l, 0, :, cols(c, CHUNK)])
        up = dot(a[t, :], wgu[l, 1, :, cols(c, CHUNK)])
        return gate, up, 0.5 * jnp.tanh(0.5 * gate) + 0.5

    def forward(c):
        def body(t):
            gate, up, sig = gates(0, c, t)
            u = (gate * sig * up).astype(BF16)
            acc[t, :] += dot(u, wdn[0, cols(c, CHUNK), :])

        tiles(body)

    def between():
        def body(t):
            h[t, :] = (h[t, :].astype(F32) + acc[t, :].astype(BF16).astype(F32)).astype(BF16)
            acc[t, :] = jnp.zeros((256, d), F32)

        tiles(body, 256)
        norm()

    def back_hidden(l, c):
        def body(t):
            gate, up, sig = gates(l, c, t)
            by_u = dot(dyb[t, :], wdn[l, cols(c, CHUNK), :], ((1,), (1,))).astype(BF16).astype(F32)
            silu = gate * sig
            act[t, :] = (silu * up).astype(BF16)
            dgu[t, CHUNK:] = (by_u * silu).astype(BF16)
            dgu[t, :CHUNK] = (by_u * up * (sig + silu * (1.0 - sig))).astype(BF16)

        tiles(body)

    def back_weights(l, c):
        for part in range(2):
            lo = part * CHUNK
            ggu[l, part, :, cols(c, CHUNK)] = dot(at[...], dgu[:, lo:lo + CHUNK]).astype(BF16)
        gdn[l, cols(c, CHUNK), :] = dot(act[...], dyb[...], ((0,), (0,))).astype(BF16)

    def back_normed(l, c):
        def body(t):
            acc[t, :] += (dot(dgu[t, :CHUNK], wgu[l, 0, :, cols(c, CHUNK)], ((1,), (1,)))
                          + dot(dgu[t, CHUNK:], wgu[l, 1, :, cols(c, CHUNK)], ((1,), (1,))))

        tiles(body)

    def back_norm():
        def body(t):
            wide = h[t, :].astype(F32)
            by_a = acc[t, :].astype(BF16).astype(F32)
            scale = lax.rsqrt(jnp.mean(wide * wide, -1, keepdims=True) + 1e-6)
            along = jnp.mean(by_a * wide, -1, keepdims=True)
            by_h = (scale * by_a - wide * (scale * scale * scale * along)).astype(BF16)
            dyb[t, :] = (dyb[t, :].astype(F32) + by_h.astype(F32)).astype(BF16)

        tiles(body, 256)

    def pass_on(term, arrived, slot, recv, send, sign, s, out, out_sem):
        def ring(src, dst, k):
            return pltpu.make_async_remote_copy(
                src_ref=src, dst_ref=dst, send_sem=send, recv_sem=recv(k), device_id={"dp": at_ring(sign)}, device_id_type=MESH)

        if s > 0:
            ring(term, arrived(s - 1), s - 1).wait_recv()
            term[...] = (term[...].astype(F32) + arrived(s - 1)[...].astype(F32)).astype(BF16)
        if s < n - 1:
            ring(term, arrived(s), s).start()
        else:
            pltpu.make_async_copy(term, out, out_sem).start()

    def scatter_gu(l, c, s):
        for way, sign, out in ((0, 1, gg_ref), (1, -1, gu_ref)):
            pass_on(
                ggu.at[l, way, span(at_ring(-sign * (1 + s)) * rows, rows), cols(c, CHUNK)],
                lambda k, way=way: rgu.at[way, l, k, :, cols(c, CHUNK)], None,
                lambda k, way=way: gu_recv.at[way, l, c, k], gu_send.at[way, l, c], sign, s,
                out.at[l, :, cols(c, CHUNK)], out_gu.at[way, l, c])

    def scatter_dn(l, v, s):
        for way, sign in ((0, 1), (1, -1)):
            pass_on(
                gdn.at[l, span(at_ring(-sign * (1 + s)) * 2 * half + way * half, half), cols(v, STRIP)],
                lambda k, way=way: rdn.at[way, l, k, :, cols(v, STRIP)], None,
                lambda k, way=way: dn_recv.at[way, l, v, k], dn_send.at[way, l, v], sign, s,
                gd_ref.at[l, pl.ds(way * half, half), cols(v, STRIP)], out_dn.at[way, l, v])

    length = 2 * chunks + strips

    def scatter(slot):
        for s in range(n):
            q = slot - s
            l, r = layers - 1 - lax.div(q, length), lax.rem(q, length)
            within = (q >= 0) & (q < layers * length)
            pl.when(within & (r < 2 * chunks) & (lax.rem(r, 2) == 0))(lambda l=l, r=r, s=s: scatter_gu(l, lax.div(r, 2), s))
            pl.when(within & (r >= 2 * chunks))(lambda l=l, r=r, s=s: scatter_dn(l, r - 2 * chunks, s))

    first = strips + far
    turn = first + pieces
    again = 2 * chunks + 3
    last = turn + 1 + layers * length + n - 1

    @pl.loop(0, last)
    def _(i):
        o = i - turn
        even = lax.rem(o + turn * 2, 2) == 0

        gslot = jnp.where(o < 0, i, turn + lax.div(o, 2))
        pl.when((o < 0) | ((o < 2 * chunks) & even))(lambda: gather(gslot))

        @pl.when(i == 1)
        def _():
            load_x.wait()
            norm()

        pl.when(i == 2)(zero)

        @pl.when(i == first)
        def _():
            need_strips(0)

        @pl.when((i >= first) & (i < first + chunks))
        def _():
            need_chunk(0, i - first)
            forward(i - first)

        pl.when(i == first + chunks)(between)

        @pl.when(o == -1)
        def _():
            transpose()

        pl.when(o == 0)(lambda: need_strips(1))

        second = (o >= 0) & (o < 2 * chunks)
        firsts = (o >= again) & (o < again + 2 * chunks)
        l = jnp.where(second, 1, 0)
        w = jnp.where(second, o, o - again)
        c = lax.div(w, 2)
        pl.when(second & (lax.rem(w, 2) == 0))(lambda: need_chunk(1, c))
        pl.when((second | firsts) & (lax.rem(w, 2) == 0))(lambda: back_hidden(l, c))
        pl.when((second | firsts) & (lax.rem(w, 2) == 1))(lambda: back_weights(l, c))
        pl.when(second & (lax.rem(w, 2) == 1))(lambda: back_normed(1, c))

        @pl.when(o == 2 * chunks)
        def _():
            back_norm()
            load_x.start()

        @pl.when(o == 2 * chunks + 1)
        def _():
            load_x.wait()
            norm()

        pl.when(o == 2 * chunks + 2)(transpose)
        pl.when(o >= 1)(lambda: scatter(o - 1))

    @pl.loop(0, layers)
    def _(l):
        @pl.loop(0, strips)
        def _(k):
            j = l * pieces + k
            all_of(ag_send.at[j], ag_recv.at[0, j, 0], True).wait_send()
            all_of(pair_send.at[j], ag_recv.at[0, j, 0], True).wait_send()
            for way in range(2):
                all_of(dn_send.at[way, l, k], ag_recv.at[0, j, 0], True).wait_send()
                pltpu.make_async_copy(gdn.at[0, pl.ds(0, half), pl.ds(0, STRIP)], gd_ref.at[0, pl.ds(0, half), pl.ds(0, STRIP)],
                                      out_dn.at[way, l, k]).wait()

        @pl.loop(0, chunks)
        def _(c):
            j = l * pieces + strips + c
            all_of(ag_send.at[j], ag_recv.at[0, j, 0], False).wait_send()
            all_of(pair_send.at[j], ag_recv.at[0, j, 0], False).wait_send()
            for way in range(2):
                all_of(gu_send.at[way, l, c], ag_recv.at[0, j, 0], False).wait_send()
                pltpu.make_async_copy(ggu.at[0, 0, pl.ds(0, rows), pl.ds(0, CHUNK)], gg_ref.at[0, :, pl.ds(0, CHUNK)],
                                      out_gu.at[way, l, c]).wait()


def gradients(n, x, dy, wg, wu, wd):
    layers, rows, ff = wg.shape
    half, d = wd.shape[1] // 2, wd.shape[2]
    tokens = x.shape[1]
    chunks, strips = ff // CHUNK, d // STRIP
    pieces = chunks + strips
    dma = pltpu.SemaphoreType.DMA
    anywhere = pl.BlockSpec(memory_space=pl.ANY)
    return pl.pallas_call(
        functools.partial(kernel, n),
        out_shape=[jax.ShapeDtypeStruct(w.shape, BF16) for w in (wg, wu, wd)],
        in_specs=[anywhere] * 5,
        out_specs=[anywhere] * 3,
        scratch_shapes=[
            pltpu.VMEM((tokens, d), BF16),
            pltpu.VMEM((tokens, d), BF16),
            pltpu.VMEM((d, tokens), BF16),
            pltpu.VMEM((tokens, d), BF16),
            pltpu.VMEM((layers, 2, d, ff), BF16),
            pltpu.VMEM((layers, ff, d), BF16),
            pltpu.VMEM((layers, 2, d, ff), BF16),
            pltpu.VMEM((layers, ff, d), BF16),
            pltpu.VMEM((2, layers, n - 1, rows, ff), BF16),
            pltpu.VMEM((2, layers, n - 1, half, d), BF16),
            pltpu.VMEM((tokens, d), F32),
            pltpu.VMEM((tokens, 2 * CHUNK), BF16),
            pltpu.VMEM((tokens, CHUNK), BF16),
            dma((3 * layers + 1,)),
            dma,
            dma((2, layers * pieces, n // 2)),
            dma((layers * pieces,)),
            dma((layers * pieces,)),
            dma((layers * pieces,)),
            dma((2, layers, chunks, n - 1)),
            dma((2, layers, chunks)),
            dma((2, layers, strips, n - 1)),
            dma((2, layers, strips)),
            dma((2, layers, chunks)),
            dma((2, layers, strips)),
        ],
        compiler_params=pltpu.CompilerParams(collective_id=0, has_side_effects=True, vmem_limit_bytes=VMEM_BYTES),
    )(x, dy, wg, wu, wd)


def adamw(w, m, v, g):
    m = 0.9 * m + 0.1 * g
    v = 0.95 * v + 0.05 * g * g
    step = m * lax.rsqrt(v + 1e-8) + 0.1 * w
    return (w - 0.02 * step).astype(jnp.bfloat16), m, v


def solution(mesh):
    n = mesh.shape["dp"]

    def step(x, dy, *arrays):
        weights, m, v = (arrays[i : i + 3] for i in (0, 3, 6))
        grads = gradients(n, x, dy, *weights)
        new = [adamw(w.astype(F32), m, v, g.astype(F32)) for w, m, v, g in zip(weights, m, v, grads, strict=True)]
        return tuple(one[which] for which in range(3) for one in new)

    states, cut = P(("rep", "dp"), None, None), P(None, "dp", None)
    return jax.shard_map(
        step,
        mesh=mesh,
        in_specs=(states, states) + (cut,) * 9,
        out_specs=(P("rep", "dp", None),) * 9,
        check_vma=False,
    )
```

```python
import functools

import jax
import jax.numpy as jnp
from jax import lax
from jax.experimental import pallas as pl
from jax.experimental.pallas import tpu as pltpu
from jax.sharding import PartitionSpec as P

MESH = pl.DeviceIdType.MESH
F32, BF16 = jnp.float32, jnp.bfloat16
CHUNK = 256
STRIP = 128
TILE = 512
GATHER_LAG = 1
SUM_LAG = 3
VMEM_BYTES = 67043328


def dot(a, b, dims=((1,), (0,))):
    return lax.dot_general(a, b, (dims, ((), ())), preferred_element_type=F32)


def kernel(n, x_ref, dy_ref, wg_ref, wu_ref, wd_ref, gg_ref, gu_ref, gd_ref,
           h, a, at, dyb, wgu, wdn, ggu, gdn, rgu, rdn, acc, dgu, act,
           local_sem, x_sem, ag_recv, ag_send, pair_recv, pair_send, gu_recv, gu_send, dn_recv, dn_send, out_gu, out_dn):
    layers, rows, ff = wg_ref.shape
    half = wd_ref.shape[1] // 2
    tokens, d = h.shape
    chunks, strips = ff // CHUNK, d // STRIP
    pieces = 1 + chunks
    far = n // 2
    z = lax.axis_index("dp")
    me = lax.axis_index("rep")
    core = lax.rem(me, 2)
    partner = me + 1 - 2 * core

    def at_ring(k):
        return lax.rem(z + 2 * n + k, n)

    def cols(c, width):
        return pl.ds(pl.multiple_of(c * width, width), width)

    def span(start, size):
        return pl.ds(pl.multiple_of(start, 16), size)

    loads = []
    for l in range(layers):
        loads.append((wg_ref.at[l], wgu.at[l, 0, span(z * rows, rows)]))
        loads.append((wu_ref.at[l], wgu.at[l, 1, span(z * rows, rows)]))
        loads.append((wd_ref.at[l], wdn.at[l, span(z * 2 * half, 2 * half)]))
    loads.append((dy_ref.at[0], dyb))
    loads = [pltpu.make_async_copy(src, dst, local_sem.at[i]) for i, (src, dst) in enumerate(loads)]
    load_x = pltpu.make_async_copy(x_ref.at[0], h, x_sem)
    for load in loads:
        load.start()
    load_x.start()

    barrier = pltpu.get_barrier_semaphore()
    for step in (1, -1):
        pl.semaphore_signal(barrier, inc=1, device_id={"dp": at_ring(step)}, device_id_type=MESH)
    pl.semaphore_signal(barrier, inc=1, device_id={"rep": partner}, device_id_type=MESH)
    pl.semaphore_wait(barrier, 3)
    for load in loads:
        load.wait()

    def block(l, k, down, origin, count=1):
        if down:
            return wdn.at[l, span(origin * 2 * half + core * half, half * count)]
        return wgu.at[l, core, span(origin * rows, rows * count), cols(k - 1, CHUNK)]

    def hop(l, k, j, down, s):
        for way, sign in ((0, 1), (1, -1)):
            ref = block(l, k, down, at_ring(-sign * s))

            def ring(slot):
                return pltpu.make_async_remote_copy(
                    src_ref=ref, dst_ref=ref, send_sem=ag_send.at[j], recv_sem=ag_recv.at[way, j, slot],
                    device_id={"dp": at_ring(sign)}, device_id_type=MESH)

            def arrive():
                ring(s - 1).wait_recv()

            def send():
                ring(s).start()

            def share():
                pltpu.make_async_remote_copy(
                    src_ref=ref, dst_ref=ref, send_sem=pair_send.at[j], recv_sem=pair_recv.at[j],
                    device_id={"rep": partner}, device_id_type=MESH).start()

            if s == 0:
                send()
            elif s < far - 1:
                arrive()
                send()
                share()
            elif s == far - 1:
                arrive()
                pl.when(lax.rem(j, 2) == way)(send)
                share()
            else:
                @pl.when(lax.rem(j, 2) == way)
                def _():
                    arrive()
                    share()

    def gather(slot):
        for s in range(far + 1):
            j = slot - GATHER_LAG * s
            l, k = lax.div(j, pieces), lax.rem(j, pieces)
            pl.when((j >= 0) & (j < layers * pieces) & (k < 1))(functools.partial(hop, l, k, j, True, s))
            pl.when((j >= 0) & (j < layers * pieces) & (k >= 1))(functools.partial(hop, l, k, j, False, s))

    def all_of(sem_send, sem_recv, down):
        ref = wdn.at[0, pl.ds(0, (n - 1) * half)] if down else wgu.at[0, 0, pl.ds(0, (n - 1) * rows), pl.ds(0, CHUNK)]
        return pltpu.make_async_remote_copy(
            src_ref=ref, dst_ref=ref, send_sem=sem_send, recv_sem=sem_recv, device_id={"rep": partner}, device_id_type=MESH)

    def need_down(l):
        j = l * pieces
        all_of(pair_send.at[j], pair_recv.at[j], True).wait_recv()

    def need_chunk(l, c):
        j = l * pieces + 1 + c
        all_of(pair_send.at[j], pair_recv.at[j], False).wait_recv()

    def tiles(body, size=TILE, part=0, parts=1):
        steps = tokens // size // parts

        @pl.loop(part * steps, part * steps + steps)
        def _(i):
            body(pl.ds(pl.multiple_of(i * size, size), size))

    def norm():
        def body(t):
            wide = h[t, :].astype(F32)
            scale = lax.rsqrt(jnp.mean(wide * wide, -1, keepdims=True) + 1e-6)
            a[t, :] = (wide * scale).astype(BF16)

        tiles(body, 256)

    def transpose():
        tiles(lambda t: at.__setitem__((slice(None), t), a[t, :].T), 256)

    def zero():
        def body(t):
            acc[t, :] = jnp.zeros((TILE, d), F32)

        tiles(body)

    def gates(l, c, t):
        gate = dot(a[t, :], wgu[l, 0, :, cols(c, CHUNK)])
        up = dot(a[t, :], wgu[l, 1, :, cols(c, CHUNK)])
        return gate, up, 0.5 * jnp.tanh(0.5 * gate) + 0.5

    def forward(c):
        def body(t):
            gate, up, sig = gates(0, c, t)
            u = (gate * sig * up).astype(BF16)
            acc[t, :] += dot(u, wdn[0, cols(c, CHUNK), :])

        tiles(body)

    def between():
        def body(t):
            h[t, :] = (h[t, :].astype(F32) + acc[t, :].astype(BF16).astype(F32)).astype(BF16)
            acc[t, :] = jnp.zeros((256, d), F32)

        tiles(body, 256)
        norm()

    def back_hidden(l, c, part):
        def body(t):
            gate, up, sig = gates(l, c, t)
            by_u = dot(dyb[t, :], wdn[l, cols(c, CHUNK), :], ((1,), (1,))).astype(BF16).astype(F32)
            silu = gate * sig
            act[t, :] = (silu * up).astype(BF16)
            dgu[t, CHUNK:] = (by_u * silu).astype(BF16)
            dgu[t, :CHUNK] = (by_u * up * (sig + silu * (1.0 - sig))).astype(BF16)

        tiles(body, part=part, parts=2)

    def back_weights(l, c):
        ggu[l, c] = dot(at[...], dgu[...]).astype(BF16)
        gdn[l, cols(c, CHUNK), :] = dot(act[...], dyb[...], ((0,), (0,))).astype(BF16)

    def back_normed(l, c):
        def body(t):
            acc[t, :] += (dot(dgu[t, :CHUNK], wgu[l, 0, :, cols(c, CHUNK)], ((1,), (1,)))
                          + dot(dgu[t, CHUNK:], wgu[l, 1, :, cols(c, CHUNK)], ((1,), (1,))))

        tiles(body)

    def back_norm():
        def body(t):
            wide = h[t, :].astype(F32)
            by_a = acc[t, :].astype(BF16).astype(F32)
            scale = lax.rsqrt(jnp.mean(wide * wide, -1, keepdims=True) + 1e-6)
            along = jnp.mean(by_a * wide, -1, keepdims=True)
            by_h = (scale * by_a - wide * (scale * scale * scale * along)).astype(BF16)
            dyb[t, :] = (dyb[t, :].astype(F32) + by_h.astype(F32)).astype(BF16)

        tiles(body, 256)

    def pass_on(odd, s, term, arrived, recv, send, outs):
        up = n - 1 - far if odd else far
        ways = ((1, up, 0), (-1, n - 1 - up, up))

        def ring(sign, k, src):
            return pltpu.make_async_remote_copy(
                src_ref=src, dst_ref=arrived(k), send_sem=send, recv_sem=recv(k), device_id={"dp": at_ring(sign)}, device_id_type=MESH)

        if s < far:
            for sign, hops, base in ways:
                if s < hops:
                    block = term(at_ring(sign * (hops - s)))
                    if s > 0:
                        k = base + s - 1
                        ring(sign, k, block).wait_recv()
                        block[...] = (block[...].astype(F32) + arrived(k)[...].astype(F32)).astype(BF16)
                    ring(sign, base + s, block).start()
        else:
            mine = term(z)
            total = mine[...].astype(F32)
            for sign, hops, base in ways:
                k = base + hops - 1
                ring(sign, k, mine).wait_recv()
                total = total + arrived(k)[...].astype(F32)
            mine[...] = total.astype(BF16)
            for part, (out, sem) in enumerate(outs):
                pltpu.make_async_copy(mine.at[:, pl.ds(part * CHUNK, CHUNK)] if len(outs) > 1 else mine, out, sem).start()

    def scatter_gu(odd, l, c, s):
        pass_on(
            odd, s, lambda b: ggu.at[l, c, span(b * rows, rows)], lambda k: rgu.at[l, c, k], lambda k: gu_recv.at[l, c, k], gu_send.at[l, c],
            [(gg_ref.at[l, :, cols(c, CHUNK)], out_gu.at[0, l, c]), (gu_ref.at[l, :, cols(c, CHUNK)], out_gu.at[1, l, c])])

    def scatter_dn(odd, l, v, s):
        pass_on(
            odd, s, lambda b: gdn.at[l, span(b * 2 * half, 2 * half), cols(v, STRIP)], lambda k: rdn.at[l, k, :, cols(v, STRIP)],
            lambda k: dn_recv.at[l, v, k], dn_send.at[l, v], [(gd_ref.at[l, :, cols(v, STRIP)], out_dn.at[l, v])])

    length = 4 * chunks + 2 * strips

    def scatter(slot):
        for s in range(far + 1):
            q = slot - SUM_LAG * s
            l, r = layers - 1 - lax.div(q, length), lax.rem(q, length)
            within = (q >= 0) & (q < layers * length)
            for odd in range(2):
                pl.when(within & (r < 4 * chunks) & (lax.rem(r, 8) == 4 * odd))(
                    functools.partial(scatter_gu, odd, l, lax.div(r, 4), s))
                pl.when(within & (r >= 4 * chunks) & (lax.rem(r - 4 * chunks + 4, 4) == 2 * odd))(
                    functools.partial(scatter_dn, odd, l, lax.div(r - 4 * chunks, 2), s))

    first = 1 + GATHER_LAG * far
    turn = first + pieces
    again = 4 * chunks + 3
    last = turn + 2 + layers * length + SUM_LAG * far

    @pl.loop(0, last)
    def _(i):
        o = i - turn
        quarter = lax.rem(o + 4 * turn, 4)

        gslot = jnp.where(o < 0, i, turn + lax.div(o, 4))
        pl.when((o < 0) | ((o < 4 * chunks) & (quarter == 0)))(lambda: gather(gslot))

        @pl.when(i == 1)
        def _():
            load_x.wait()
            norm()

        pl.when(i == 2)(zero)

        @pl.when(i == first)
        def _():
            need_down(0)

        @pl.when((i >= first) & (i < first + chunks))
        def _():
            need_chunk(0, i - first)
            forward(i - first)

        pl.when(i == first + chunks)(between)
        pl.when(i == first + chunks + 1)(transpose)
        pl.when(o == 0)(lambda: need_down(1))

        second = (o >= 0) & (o < 4 * chunks)
        firsts = (o >= again) & (o < again + 4 * chunks)
        l = jnp.where(second, 1, 0)
        w = jnp.where(second, o, o - again)
        c, step = lax.div(w, 4), lax.rem(w, 4)
        pl.when(second & (step == 0))(lambda: need_chunk(1, c))
        pl.when((second | firsts) & (step < 2))(lambda: back_hidden(l, c, step))
        pl.when((second | firsts) & (step == 2))(lambda: back_weights(l, c))
        pl.when(second & (step == 3))(lambda: back_normed(1, c))

        @pl.when(o == 4 * chunks)
        def _():
            back_norm()
            load_x.start()

        @pl.when(o == 4 * chunks + 1)
        def _():
            load_x.wait()
            norm()

        pl.when(o == 4 * chunks + 2)(transpose)
        pl.when(o >= 2)(lambda: scatter(o - 2))

    def sent(ref, sem):
        pltpu.make_async_remote_copy(
            src_ref=ref, dst_ref=ref, send_sem=sem, recv_sem=x_sem, device_id={"rep": partner}, device_id_type=MESH).wait_send()

    @pl.loop(0, layers)
    def _(l):
        @pl.loop(0, strips)
        def _(v):
            sent(rdn.at[0, :, :, pl.ds(0, STRIP)], dn_send.at[l, v])
            pltpu.make_async_copy(gdn.at[0, pl.ds(0, 2 * half), pl.ds(0, STRIP)], gd_ref.at[0, :, pl.ds(0, STRIP)], out_dn.at[l, v]).wait()

        @pl.loop(0, chunks)
        def _(c):
            sent(rgu.at[0, 0], gu_send.at[l, c])
            for part in range(2):
                pltpu.make_async_copy(ggu.at[0, 0, pl.ds(0, rows), pl.ds(0, CHUNK)], gg_ref.at[0, :, pl.ds(0, CHUNK)],
                                      out_gu.at[part, l, c]).wait()

        all_of(ag_send.at[l * pieces], x_sem, True).wait_send()
        all_of(pair_send.at[l * pieces], x_sem, True).wait_send()

        @pl.loop(l * pieces + 1, l * pieces + pieces)
        def _(j):
            all_of(ag_send.at[j], x_sem, False).wait_send()
            all_of(pair_send.at[j], x_sem, False).wait_send()


def gradients(n, x, dy, wg, wu, wd):
    layers, rows, ff = wg.shape
    half, d = wd.shape[1] // 2, wd.shape[2]
    tokens = x.shape[1]
    chunks, strips = ff // CHUNK, d // STRIP
    pieces = 1 + chunks
    dma = pltpu.SemaphoreType.DMA
    anywhere = pl.BlockSpec(memory_space=pl.ANY)
    return pl.pallas_call(
        functools.partial(kernel, n),
        out_shape=[jax.ShapeDtypeStruct(w.shape, BF16) for w in (wg, wu, wd)],
        in_specs=[anywhere] * 5,
        out_specs=[anywhere] * 3,
        scratch_shapes=[
            pltpu.VMEM((tokens, d), BF16),
            pltpu.VMEM((tokens, d), BF16),
            pltpu.VMEM((d, tokens), BF16),
            pltpu.VMEM((tokens, d), BF16),
            pltpu.VMEM((layers, 2, d, ff), BF16),
            pltpu.VMEM((layers, ff, d), BF16),
            pltpu.VMEM((layers, chunks, d, 2 * CHUNK), BF16),
            pltpu.VMEM((layers, ff, d), BF16),
            pltpu.VMEM((layers, chunks, n - 1, rows, 2 * CHUNK), BF16),
            pltpu.VMEM((layers, n - 1, 2 * half, d), BF16),
            pltpu.VMEM((tokens, d), F32),
            pltpu.VMEM((tokens, 2 * CHUNK), BF16),
            pltpu.VMEM((tokens, CHUNK), BF16),
            dma((3 * layers + 1,)),
            dma,
            dma((2, layers * pieces, n // 2)),
            dma((layers * pieces,)),
            dma((layers * pieces,)),
            dma((layers * pieces,)),
            dma((layers, chunks, n - 1)),
            dma((layers, chunks)),
            dma((layers, strips, n - 1)),
            dma((layers, strips)),
            dma((2, layers, chunks)),
            dma((layers, strips)),
        ],
        compiler_params=pltpu.CompilerParams(collective_id=0, has_side_effects=True, vmem_limit_bytes=VMEM_BYTES),
    )(x, dy, wg, wu, wd)


def adamw(w, m, v, g):
    m = 0.9 * m + 0.1 * g
    v = 0.95 * v + 0.05 * g * g
    step = m * lax.rsqrt(v + 1e-8) + 0.1 * w
    return (w - 0.02 * step).astype(jnp.bfloat16), m, v


def solution(mesh):
    n = mesh.shape["dp"]

    def step(x, dy, *arrays):
        weights, m, v = (arrays[i : i + 3] for i in (0, 3, 6))
        grads = gradients(n, x, dy, *weights)
        new = [adamw(w.astype(F32), m, v, g.astype(F32)) for w, m, v, g in zip(weights, m, v, grads, strict=True)]
        return tuple(one[which] for which in range(3) for one in new)

    states, cut = P(("rep", "dp"), None, None), P(None, "dp", None)
    return jax.shard_map(
        step,
        mesh=mesh,
        in_specs=(states, states) + (cut,) * 9,
        out_specs=(P("rep", "dp", None),) * 9,
        check_vma=False,
    )
```

```python
import functools

import jax
import jax.numpy as jnp
from jax import lax
from jax.experimental import pallas as pl
from jax.experimental.pallas import tpu as pltpu
from jax.sharding import PartitionSpec as P

MESH = pl.DeviceIdType.MESH
F32, BF16 = jnp.float32, jnp.bfloat16
CHUNK = 256
STRIP = 128
TILE = 512
GATHER_LAG = 1
SUM_LAG = 3
VMEM_BYTES = 67043328


def dot(a, b, dims=((1,), (0,))):
    return lax.dot_general(a, b, (dims, ((), ())), preferred_element_type=F32)


def kernel(n, x_ref, dy_ref, wg_ref, wu_ref, wd_ref, gg_ref, gu_ref, gd_ref,
           h, a, at, dyb, wgu, wdn, ggu, gdn, rgu, rdn, acc, dgu, act,
           local_sem, x_sem, ag_recv, ag_send, pair_recv, pair_send, gu_recv, gu_send, dn_recv, dn_send, out_gu, out_dn):
    layers, rows, ff = wg_ref.shape
    half = wd_ref.shape[1] // 2
    tokens, d = h.shape
    chunks, strips = ff // CHUNK, d // STRIP
    pieces = 1 + chunks
    far = n // 2
    z = lax.axis_index("dp")
    me = lax.axis_index("rep")
    core = lax.rem(me, 2)
    partner = me + 1 - 2 * core

    def at_ring(k):
        return lax.rem(z + 2 * n + k, n)

    def cols(c, width):
        return pl.ds(pl.multiple_of(c * width, width), width)

    def span(start, size):
        return pl.ds(pl.multiple_of(start, 16), size)

    loads = []
    for l in range(layers):
        loads.append((wg_ref.at[l], wgu.at[l, 0, span(z * rows, rows)]))
        loads.append((wu_ref.at[l], wgu.at[l, 1, span(z * rows, rows)]))
        loads.append((wd_ref.at[l], wdn.at[l, span(z * 2 * half, 2 * half)]))
    loads.append((dy_ref.at[0], dyb))
    loads = [pltpu.make_async_copy(src, dst, local_sem.at[i]) for i, (src, dst) in enumerate(loads)]
    load_x = pltpu.make_async_copy(x_ref.at[0], h, x_sem)
    for load in loads:
        load.start()
    load_x.start()

    barrier = pltpu.get_barrier_semaphore()
    for step in (1, -1):
        pl.semaphore_signal(barrier, inc=1, device_id={"dp": at_ring(step)}, device_id_type=MESH)
    pl.semaphore_signal(barrier, inc=1, device_id={"rep": partner}, device_id_type=MESH)
    pl.semaphore_wait(barrier, 3)
    for load in loads:
        load.wait()

    def block(l, k, down, origin, count=1):
        if down:
            return wdn.at[l, span(origin * 2 * half + core * half, half * count)]
        return wgu.at[l, core, span(origin * rows, rows * count), cols(k - 1, CHUNK)]

    def hop(l, k, j, down, s):
        for way, sign in ((0, 1), (1, -1)):
            ref = block(l, k, down, at_ring(-sign * s))

            def ring(slot):
                return pltpu.make_async_remote_copy(
                    src_ref=ref, dst_ref=ref, send_sem=ag_send.at[j], recv_sem=ag_recv.at[way, j, slot],
                    device_id={"dp": at_ring(sign)}, device_id_type=MESH)

            def arrive():
                ring(s - 1).wait_recv()

            def send():
                ring(s).start()

            def share():
                pltpu.make_async_remote_copy(
                    src_ref=ref, dst_ref=ref, send_sem=pair_send.at[j], recv_sem=pair_recv.at[j],
                    device_id={"rep": partner}, device_id_type=MESH).start()

            if s == 0:
                send()
            elif s < far - 1:
                arrive()
                send()
                share()
            elif s == far - 1:
                arrive()
                pl.when(lax.rem(j, 2) == way)(send)
                share()
            else:
                @pl.when(lax.rem(j, 2) == way)
                def _():
                    arrive()
                    share()

    def gather(slot, hops):
        for s in hops:
            j = slot - GATHER_LAG * s
            l, k = lax.div(j, pieces), lax.rem(j, pieces)
            pl.when((j >= 0) & (j < layers * pieces) & (k < 1))(functools.partial(hop, l, k, j, True, s))
            pl.when((j >= 0) & (j < layers * pieces) & (k >= 1))(functools.partial(hop, l, k, j, False, s))

    def all_of(sem_send, sem_recv, down):
        ref = wdn.at[0, pl.ds(0, (n - 1) * half)] if down else wgu.at[0, 0, pl.ds(0, (n - 1) * rows), pl.ds(0, CHUNK)]
        return pltpu.make_async_remote_copy(
            src_ref=ref, dst_ref=ref, send_sem=sem_send, recv_sem=sem_recv, device_id={"rep": partner}, device_id_type=MESH)

    def need_down(l):
        j = l * pieces
        all_of(pair_send.at[j], pair_recv.at[j], True).wait_recv()

    def need_chunk(l, c):
        j = l * pieces + 1 + c
        all_of(pair_send.at[j], pair_recv.at[j], False).wait_recv()

    def tiles(body, size=TILE, part=0, parts=1):
        steps = tokens // size // parts

        @pl.loop(part * steps, part * steps + steps)
        def _(i):
            body(pl.ds(pl.multiple_of(i * size, size), size))

    def norm():
        def body(t):
            wide = h[t, :].astype(F32)
            scale = lax.rsqrt(jnp.mean(wide * wide, -1, keepdims=True) + 1e-6)
            a[t, :] = (wide * scale).astype(BF16)

        tiles(body, 256)

    def transpose():
        tiles(lambda t: at.__setitem__((slice(None), t), a[t, :].T), 256)

    def zero():
        def body(t):
            acc[t, :] = jnp.zeros((TILE, d), F32)

        tiles(body)

    def gates(l, c, t):
        gate = dot(a[t, :], wgu[l, 0, :, cols(c, CHUNK)])
        up = dot(a[t, :], wgu[l, 1, :, cols(c, CHUNK)])
        return gate, up, 0.5 * jnp.tanh(0.5 * gate) + 0.5

    def forward(c, part):
        def body(t):
            gate, up, sig = gates(0, c, t)
            u = (gate * sig * up).astype(BF16)
            acc[t, :] += dot(u, wdn[0, cols(c, CHUNK), :])

        tiles(body, part=part, parts=2)

    def between():
        def body(t):
            h[t, :] = (h[t, :].astype(F32) + acc[t, :].astype(BF16).astype(F32)).astype(BF16)
            acc[t, :] = jnp.zeros((256, d), F32)

        tiles(body, 256)
        norm()

    def back_hidden(l, c, part):
        def body(t):
            gate, up, sig = gates(l, c, t)
            by_u = dot(dyb[t, :], wdn[l, cols(c, CHUNK), :], ((1,), (1,))).astype(BF16).astype(F32)
            silu = gate * sig
            act[t, :] = (silu * up).astype(BF16)
            dgu[t, CHUNK:] = (by_u * silu).astype(BF16)
            dgu[t, :CHUNK] = (by_u * up * (sig + silu * (1.0 - sig))).astype(BF16)

        tiles(body, part=part, parts=2)

    def back_weights(l, c):
        ggu[l, c] = dot(at[...], dgu[...]).astype(BF16)
        gdn[l, cols(c, CHUNK), :] = dot(act[...], dyb[...], ((0,), (0,))).astype(BF16)

    def back_normed(l, c):
        def body(t):
            acc[t, :] += (dot(dgu[t, :CHUNK], wgu[l, 0, :, cols(c, CHUNK)], ((1,), (1,)))
                          + dot(dgu[t, CHUNK:], wgu[l, 1, :, cols(c, CHUNK)], ((1,), (1,))))

        tiles(body)

    def back_norm():
        def body(t):
            wide = h[t, :].astype(F32)
            by_a = acc[t, :].astype(BF16).astype(F32)
            scale = lax.rsqrt(jnp.mean(wide * wide, -1, keepdims=True) + 1e-6)
            along = jnp.mean(by_a * wide, -1, keepdims=True)
            by_h = (scale * by_a - wide * (scale * scale * scale * along)).astype(BF16)
            dyb[t, :] = (dyb[t, :].astype(F32) + by_h.astype(F32)).astype(BF16)

        tiles(body, 256)

    def pass_on(odd, s, term, arrived, recv, send, outs):
        up = n - 1 - far if odd else far
        ways = ((1, up, 0), (-1, n - 1 - up, up))

        def ring(sign, k, src):
            return pltpu.make_async_remote_copy(
                src_ref=src, dst_ref=arrived(k), send_sem=send, recv_sem=recv(k), device_id={"dp": at_ring(sign)}, device_id_type=MESH)

        if s < far:
            for sign, hops, base in ways:
                if s < hops:
                    block = term(at_ring(sign * (hops - s)))
                    if s > 0:
                        k = base + s - 1
                        ring(sign, k, block).wait_recv()
                        block[...] = (block[...].astype(F32) + arrived(k)[...].astype(F32)).astype(BF16)
                    ring(sign, base + s, block).start()
        else:
            mine = term(z)
            total = mine[...].astype(F32)
            for sign, hops, base in ways:
                k = base + hops - 1
                ring(sign, k, mine).wait_recv()
                total = total + arrived(k)[...].astype(F32)
            mine[...] = total.astype(BF16)
            for part, (out, sem) in enumerate(outs):
                pltpu.make_async_copy(mine.at[:, pl.ds(part * CHUNK, CHUNK)] if len(outs) > 1 else mine, out, sem).start()

    def scatter_gu(odd, l, c, s):
        pass_on(
            odd, s, lambda b: ggu.at[l, c, span(b * rows, rows)], lambda k: rgu.at[l, c, k], lambda k: gu_recv.at[l, c, k], gu_send.at[l, c],
            [(gg_ref.at[l, :, cols(c, CHUNK)], out_gu.at[0, l, c]), (gu_ref.at[l, :, cols(c, CHUNK)], out_gu.at[1, l, c])])

    def scatter_dn(odd, l, v, s):
        pass_on(
            odd, s, lambda b: gdn.at[l, span(b * 2 * half, 2 * half), cols(v, STRIP)], lambda k: rdn.at[l, k, :, cols(v, STRIP)],
            lambda k: dn_recv.at[l, v, k], dn_send.at[l, v], [(gd_ref.at[l, :, cols(v, STRIP)], out_dn.at[l, v])])

    length = 4 * chunks + 2 * strips

    def scatter(slot):
        for s in range(far + 1):
            q = slot - SUM_LAG * s
            l, r = layers - 1 - lax.div(q, length), lax.rem(q, length)
            within = (q >= 0) & (q < layers * length)
            for odd in range(2):
                pl.when(within & (r < 4 * chunks) & (lax.rem(r, 8) == 4 * odd))(
                    functools.partial(scatter_gu, odd, l, lax.div(r, 4), s))
                pl.when(within & (r >= 4 * chunks) & (lax.rem(r - 4 * chunks + 4, 4) == 2 * odd))(
                    functools.partial(scatter_dn, odd, l, lax.div(r - 4 * chunks, 2), s))

    first = 1 + GATHER_LAG * far
    turn = first + pieces
    again = 4 * chunks + 3
    last = turn + 2 + layers * length + SUM_LAG * far

    @pl.loop(0, last)
    def _(i):
        o = i - turn
        quarter = lax.rem(o + 4 * turn, 4)

        early, late = range(2), range(2, far + 1)
        back = o < 4 * chunks
        aslot = jnp.where(o <= 0, i, turn + 1 + lax.div(o, 4))
        pl.when((o <= 0) | (back & (quarter == 2)))(lambda: gather(aslot, early))

        @pl.when((i > first) & (i <= first + chunks))
        def _():
            forward(i - first - 1, 1)

        bslot = jnp.where(o < 0, i, turn + lax.div(o, 4))
        pl.when((o < 0) | (back & (quarter == 0)))(lambda: gather(bslot, late))

        @pl.when(i == 1)
        def _():
            load_x.wait()
            norm()

        pl.when(i == 2)(zero)

        @pl.when(i == first)
        def _():
            need_down(0)

        @pl.when((i >= first) & (i < first + chunks))
        def _():
            need_chunk(0, i - first)
            forward(i - first, 0)

        pl.when(i == first + chunks)(between)
        pl.when(i == first + chunks + 1)(transpose)
        pl.when(o == 0)(lambda: need_down(1))

        second = (o >= 0) & (o < 4 * chunks)
        firsts = (o >= again) & (o < again + 4 * chunks)
        l = jnp.where(second, 1, 0)
        w = jnp.where(second, o, o - again)
        c, step = lax.div(w, 4), lax.rem(w, 4)
        pl.when(second & (step == 0))(lambda: need_chunk(1, c))
        pl.when((second | firsts) & (step < 2))(lambda: back_hidden(l, c, step))
        pl.when((second | firsts) & (step == 2))(lambda: back_weights(l, c))
        pl.when(second & (step == 3))(lambda: back_normed(1, c))

        @pl.when(o == 4 * chunks)
        def _():
            back_norm()
            load_x.start()

        @pl.when(o == 4 * chunks + 1)
        def _():
            load_x.wait()
            norm()

        pl.when(o == 4 * chunks + 2)(transpose)
        pl.when(o >= 2)(lambda: scatter(o - 2))

    def sent(ref, sem):
        pltpu.make_async_remote_copy(
            src_ref=ref, dst_ref=ref, send_sem=sem, recv_sem=x_sem, device_id={"rep": partner}, device_id_type=MESH).wait_send()

    @pl.loop(0, layers)
    def _(l):
        @pl.loop(0, strips)
        def _(v):
            sent(rdn.at[0, :, :, pl.ds(0, STRIP)], dn_send.at[l, v])
            pltpu.make_async_copy(gdn.at[0, pl.ds(0, 2 * half), pl.ds(0, STRIP)], gd_ref.at[0, :, pl.ds(0, STRIP)], out_dn.at[l, v]).wait()

        @pl.loop(0, chunks)
        def _(c):
            sent(rgu.at[0, 0], gu_send.at[l, c])
            for part in range(2):
                pltpu.make_async_copy(ggu.at[0, 0, pl.ds(0, rows), pl.ds(0, CHUNK)], gg_ref.at[0, :, pl.ds(0, CHUNK)],
                                      out_gu.at[part, l, c]).wait()

        all_of(ag_send.at[l * pieces], x_sem, True).wait_send()
        all_of(pair_send.at[l * pieces], x_sem, True).wait_send()

        @pl.loop(l * pieces + 1, l * pieces + pieces)
        def _(j):
            all_of(ag_send.at[j], x_sem, False).wait_send()
            all_of(pair_send.at[j], x_sem, False).wait_send()


def gradients(n, x, dy, wg, wu, wd):
    layers, rows, ff = wg.shape
    half, d = wd.shape[1] // 2, wd.shape[2]
    tokens = x.shape[1]
    chunks, strips = ff // CHUNK, d // STRIP
    pieces = 1 + chunks
    dma = pltpu.SemaphoreType.DMA
    anywhere = pl.BlockSpec(memory_space=pl.ANY)
    return pl.pallas_call(
        functools.partial(kernel, n),
        out_shape=[jax.ShapeDtypeStruct(w.shape, BF16) for w in (wg, wu, wd)],
        in_specs=[anywhere] * 5,
        out_specs=[anywhere] * 3,
        scratch_shapes=[
            pltpu.VMEM((tokens, d), BF16),
            pltpu.VMEM((tokens, d), BF16),
            pltpu.VMEM((d, tokens), BF16),
            pltpu.VMEM((tokens, d), BF16),
            pltpu.VMEM((layers, 2, d, ff), BF16),
            pltpu.VMEM((layers, ff, d), BF16),
            pltpu.VMEM((layers, chunks, d, 2 * CHUNK), BF16),
            pltpu.VMEM((layers, ff, d), BF16),
            pltpu.VMEM((layers, chunks, n - 1, rows, 2 * CHUNK), BF16),
            pltpu.VMEM((layers, n - 1, 2 * half, d), BF16),
            pltpu.VMEM((tokens, d), F32),
            pltpu.VMEM((tokens, 2 * CHUNK), BF16),
            pltpu.VMEM((tokens, CHUNK), BF16),
            dma((3 * layers + 1,)),
            dma,
            dma((2, layers * pieces, n // 2)),
            dma((layers * pieces,)),
            dma((layers * pieces,)),
            dma((layers * pieces,)),
            dma((layers, chunks, n - 1)),
            dma((layers, chunks)),
            dma((layers, strips, n - 1)),
            dma((layers, strips)),
            dma((2, layers, chunks)),
            dma((layers, strips)),
        ],
        compiler_params=pltpu.CompilerParams(collective_id=0, has_side_effects=True, vmem_limit_bytes=VMEM_BYTES),
    )(x, dy, wg, wu, wd)


def adamw(w, m, v, g):
    m = 0.9 * m + 0.1 * g
    v = 0.95 * v + 0.05 * g * g
    step = m * lax.rsqrt(v + 1e-8) + 0.1 * w
    return (w - 0.02 * step).astype(jnp.bfloat16), m, v


def solution(mesh):
    n = mesh.shape["dp"]

    def step(x, dy, *arrays):
        weights, m, v = (arrays[i : i + 3] for i in (0, 3, 6))
        grads = gradients(n, x, dy, *weights)
        new = [adamw(w.astype(F32), m, v, g.astype(F32)) for w, m, v, g in zip(weights, m, v, grads, strict=True)]
        return tuple(one[which] for which in range(3) for one in new)

    states, cut = P(("rep", "dp"), None, None), P(None, "dp", None)
    return jax.shard_map(
        step,
        mesh=mesh,
        in_specs=(states, states) + (cut,) * 9,
        out_specs=(P("rep", "dp", None),) * 9,
        check_vma=False,
    )
```
